32 devices in a mesh: tm: 8 (over z, y), chan: 4 (over x, core).
Axes of the slice: x: 2, y: 2, z: 4, core: 2. Of those that a mesh axis runs over, the one named last changes fastest.
Arguments:
- series: float32 [256, 2048], P('chan', 'tm'), may hold values from -6 to 6
- lengths: int32 [16], replicated, may hold values from 42 to 128
Outputs:
- peak: float32 [2048], P('tm')
The draws below stay inside these ranges and needn't reach their ends.
All inputs are finite; a program needn't handle non-finite values.
Results may differ from the reference program's by a relative error of at most 0.0015.
Values may be sent and summed in bfloat16 or wider, within the bound.
A program may use at most 128 MiB of HBM per device.

```python
import jax
import jax.numpy as jnp
from jax import lax

C = 256
WIN = 256
ROWS_DEV = 256
STEPS = 2
ROWS = 2048
NSEG = 16
N_TM = 8


def with_ends(drawn, own_key, low, largest):
    longest = drawn.shape.index(max(drawn.shape))
    spots = []
    for shift in (0, 1):
        where = [jax.random.randint(jax.random.fold_in(own_key, axis), (), 0, length) for axis, length in enumerate(drawn.shape)]
        where[longest] = (where[longest] + shift) % drawn.shape[longest]
        spots.append(tuple(where))
    return drawn.at[spots[0]].set(low).at[spots[1]].set(largest)


def block_scale(key, shape, shards, smallest, top_value):
    factor_of = 1.0
    for axis_at, shards_of in shards:
        draws = jax.random.uniform(jax.random.fold_in(jax.random.fold_in(key, 6), axis_at), (shards_of,), jnp.float32, smallest / len(shards), top_value / len(shards))
        factor_of = factor_of * jnp.repeat(jnp.exp(draws), shape[axis_at] // shards_of).reshape((-1,) + (1,) * (len(shape) - 1 - axis_at))
    return factor_of


def normal_values(key, extent, width, bound, pieces=(), held_as=jnp.bfloat16):
    array = jax.random.normal(key, extent, jnp.float32) * width
    if len(pieces) > 0:
        array = block_scale(key, extent, pieces, -0.22, 0.18) * array
    return jnp.clip(array, min=-bound, max=bound).astype(held_as)


def setup_inputs(seed: int = 0) -> dict:
    key_list = jax.random.split(jax.random.key(seed), 3)
    series = normal_values(key_list[0], (C, ROWS), 1.0, 6.0, ((0, 4), (1, 8)), jnp.float32)
    lengths = with_ends(jax.random.randint(key_list[1], (NSEG,), ROWS_DEV // 6, ROWS_DEV // 2 + 1), jax.random.fold_in(key_list[1], 1), ROWS_DEV // 6, (ROWS_DEV // 2 + 1) - 1).astype(jnp.int32)
    return {"series": series, "lengths": lengths}


EPS = 1e-05
MASKED = -1000000000.0

def windows_of(extended):
    count = extended.shape[1] - WIN + 1
    starts = jnp.arange(count, dtype=jnp.int32)
    index = starts[:, None] + jnp.arange(WIN, dtype=jnp.int32)[None, :]
    stacked = jnp.transpose(extended[:, index], (1, 0, 2))
    center = stacked - lax.optimization_barrier(jnp.mean(stacked, axis=2, keepdims=True))
    spread = lax.optimization_barrier(jnp.mean(center * center, axis=2, keepdims=True))
    normed = center * lax.rsqrt(spread + EPS)
    return normed.reshape(count, -1).astype(jnp.bfloat16)

def validity(block, lengths, rows, total):
    local = jnp.arange(rows, dtype=jnp.int32)
    seg_len = rows // 2
    pair = lax.dynamic_slice_in_dim(lengths, (block * 2).astype(jnp.int32), 2)
    limit = jnp.where(local < seg_len, pair[0], pair[1])
    offset = local % seg_len
    return (offset < limit) & (block * rows + local <= total - WIN)

def reference(series, lengths):
    total = series.shape[1]
    padded = jnp.concatenate([series, jnp.zeros((series.shape[0], WIN - 1), series.dtype)], axis=1)
    excl = WIN // 4

    def block_windows(block):
        start = (block * ROWS_DEV).astype(jnp.int32)
        return windows_of(lax.dynamic_slice_in_dim(padded, start, ROWS_DEV + WIN - 1, 1))

    def row_block(block):
        rows_z = block_windows(block)
        rows_ok = validity(block, lengths, ROWS_DEV, total)
        local = jnp.arange(ROWS_DEV, dtype=jnp.int32)
        best = jnp.full((ROWS_DEV,), MASKED, jnp.float32)
        for step in range(STEPS + 1):
            other = block - step
            safe = jnp.maximum(other, 0)
            cols_z = block_windows(safe)
            cols_ok = validity(safe, lengths, ROWS_DEV, total) & (other >= 0)
            score = lax.dot_general(rows_z, cols_z, (((1,), (1,)), ((), ())), preferred_element_type=jnp.float32) * (1.0 / WIN)
            lag = step * ROWS_DEV + local[:, None] - local[None, :]
            keep = rows_ok[:, None] & cols_ok[None, :] & (lag >= excl)
            best = jnp.maximum(best, lax.optimization_barrier(jnp.max(jnp.where(keep, score, MASKED), axis=1)))
        return jnp.where(best > 0.5 * MASKED, best, 0.0).astype(jnp.float32)
    blocks = lax.map(row_block, jnp.arange(N_TM, dtype=jnp.int32))
    return blocks.reshape(total)
```

```python
import functools

import jax
import jax.numpy as jnp
from jax import lax
from jax.experimental import pallas as pl
from jax.experimental.pallas import tpu as pltpu
from jax.sharding import PartitionSpec as P

WIN = 256
STEPS = 2
GROUP = 8
EPS = 1e-05
MASKED = -1000000000.0
MESH = pl.DeviceIdType.MESH


def window_stats(x):
    width = x.shape[1]
    mean, second = x, None
    span = 1
    while span < WIN:
        later = pltpu.roll(mean, width - span, 1)
        gap = later - mean
        added = gap * gap * (span * 0.5)
        second = added if second is None else second + pltpu.roll(second, width - span, 1) + added
        mean = (mean + later) * 0.5
        span *= 2
    return mean, lax.rsqrt(second * (1.0 / WIN) + EPS)


def kernel(n_tm, n_chan, lengths, series, out, halo, xw, mu, sc, zown, zbuf, acc, recvbuf, peaks,
           halo_send, halo_recv, part_send, part_recv, peak_send, peak_recv):
    depth, rows = series.shape
    own = rows // n_chan
    total = rows * n_tm
    excl = WIN // 4
    block = lax.axis_index("tm")
    part = lax.axis_index("chan")

    def at(distance):
        return lax.rem(block + distance + n_tm, n_tm)

    def peer(d):
        return lax.rem(part + d, n_chan)

    barrier = pltpu.get_barrier_semaphore()
    greet = [(at(d), part) for d in (1, -1, -2)] + [(block, peer(d)) for d in range(1, n_chan)]
    for target in greet:
        pl.semaphore_signal(barrier, inc=1, device_id=target, device_id_type=MESH)
    pl.semaphore_wait(barrier, len(greet))

    halo_copies = []
    for slot, distance in enumerate((-1, 1, 2)):
        copy = pltpu.make_async_remote_copy(
            src_ref=series, dst_ref=halo.at[slot], send_sem=halo_send.at[slot], recv_sem=halo_recv.at[slot],
            device_id=(at(distance), part), device_id_type=MESH)
        copy.start()
        halo_copies.append(copy)

    def build_channel(r, x8, mu8, sc8, store):
        width = x8.shape[1]
        row = jnp.broadcast_to(x8[r:r + 1, :], (16, width))
        spread = pltpu.roll(row, width - 15, 1, stride=1, stride_axis=0)
        m = jnp.broadcast_to(mu8[r:r + 1, :], (16, rows))
        s = jnp.broadcast_to(sc8[r:r + 1, :], (16, rows))
        for q in range(8):
            moved = spread if q == 0 else pltpu.roll(spread, width - 16 * q, 1)
            for half in range(WIN // 128):
                z = (moved[:, 128 * half:128 * half + rows] - m) * s
                store(128 * half + 16 * q, z.astype(jnp.bfloat16))

    def stage(step):
        if step == 0:
            halo_copies[0].wait_recv()
            after = jnp.where(block == n_tm - 1, 0.0, halo[0])
            here = series[...]
        else:
            halo_copies[step].wait_recv()
            here = halo[step]
            after = series[...] if step == 1 else halo[1]
        x = jnp.concatenate([here, after], axis=1)
        xw[...] = x
        mean, scale = window_stats(x)
        mu[...] = mean[:, :rows]
        sc[...] = scale[:, :rows]

        acc[step] = jnp.zeros((rows, rows), jnp.float32)

        def group(g, carry):
            rows8 = pl.ds(pl.multiple_of(g * GROUP, GROUP), GROUP)
            x8, mu8, sc8 = xw[rows8, :], mu[rows8, :], sc[rows8, :]
            for r in range(GROUP):
                def store(k, value, r=r):
                    zbuf[r * WIN + k:r * WIN + k + 16, :] = value
                build_channel(r, x8, mu8, sc8, store)
            if step == 0:
                zown[g] = zbuf[...].T
            acc[step] += jnp.dot(zown[g], zbuf[...], preferred_element_type=jnp.float32)
            return carry

        lax.fori_loop(0, depth // GROUP, group, 0)

        copies = []
        for d in range(1, n_chan):
            copy = pltpu.make_async_remote_copy(
                src_ref=acc.at[step, pl.ds(pl.multiple_of(peer(d) * own, own), own), :],
                dst_ref=recvbuf.at[step, d - 1],
                send_sem=part_send.at[step, d - 1], recv_sem=part_recv.at[step, d - 1],
                device_id=(block, peer(d)), device_id_type=MESH)
            copy.start()
            copies.append(copy)
        return copies

    sent = [stage(step) for step in range(STEPS + 1)]

    seg_len = rows // 2
    row_at = part * own + lax.broadcasted_iota(jnp.int32, (own, rows), 0)
    col_at = lax.broadcasted_iota(jnp.int32, (own, rows), 1)

    def valid(which, local):
        limit = jnp.where(local < seg_len, lengths[which * 2], lengths[which * 2 + 1])
        offset = jnp.where(local < seg_len, local, local - seg_len)
        return (offset < limit) & (which * rows + local <= total - WIN)

    rows_ok = valid(block, row_at)
    best = jnp.full((own, rows), MASKED, jnp.float32)
    for step in range(STEPS + 1):
        other = block - step
        safe = jnp.maximum(other, 0)
        keep = rows_ok & valid(safe, col_at) & (other >= 0) & (step * rows + row_at - col_at >= excl)
        summed = acc[step, pl.ds(pl.multiple_of(part * own, own), own), :]
        for d in range(1, n_chan):
            sent[step][d - 1].wait_recv()
            summed = summed + recvbuf[step, d - 1]
        best = jnp.maximum(best, jnp.where(keep, summed * (1.0 / WIN), MASKED))
    folded = best[:, :128]
    for at_lane in range(128, rows, 128):
        folded = jnp.maximum(folded, best[:, at_lane:at_lane + 128])
    top = jnp.max(folded.T, axis=0, keepdims=True)
    top = jnp.where(top > 0.5 * MASKED, top, 0.0)
    padded = jnp.concatenate([top, jnp.zeros((1, 128 - own), jnp.float32)], axis=1)
    peaks[0] = jnp.broadcast_to(padded, (8, 128))
    copies = []
    for d in range(1, n_chan):
        copy = pltpu.make_async_remote_copy(
            src_ref=peaks.at[0], dst_ref=peaks.at[d],
            send_sem=peak_send.at[d - 1], recv_sem=peak_recv.at[d - 1],
            device_id=(block, peer(d)), device_id_type=MESH)
        copy.start()
        copies.append(copy)
    for copy in copies:
        copy.wait_recv()
    slots = [peaks[d, 0:1, :own] for d in range(n_chan)]
    pieces = []
    for q in range(n_chan):
        piece = slots[0]
        for d in range(1, n_chan):
            piece = jnp.where(lax.rem(part + n_chan - d, n_chan) == q, slots[d], piece)
        pieces.append(piece)
    out[...] = jnp.concatenate(pieces, axis=1)

    for copy in halo_copies + [c for step in sent for c in step] + copies:
        copy.wait_send()


def solution(mesh):
    n_tm, n_chan = mesh.shape["tm"], mesh.shape["chan"]

    def body(series, lengths):
        depth, rows = series.shape
        own = rows // n_chan
        vmem = pl.BlockSpec(memory_space=pltpu.VMEM)
        peak = pl.pallas_call(
            functools.partial(kernel, n_tm, n_chan),
            out_shape=jax.ShapeDtypeStruct((1, rows), jnp.float32),
            in_specs=[pl.BlockSpec(memory_space=pltpu.SMEM), vmem],
            out_specs=vmem,
            scratch_shapes=[
                pltpu.VMEM((STEPS + 1, depth, rows), jnp.float32),
                pltpu.VMEM((depth, 2 * rows), jnp.float32),
                pltpu.VMEM((depth, rows), jnp.float32),
                pltpu.VMEM((depth, rows), jnp.float32),
                pltpu.VMEM((depth // GROUP, rows, GROUP * WIN), jnp.bfloat16),
                pltpu.VMEM((GROUP * WIN, rows), jnp.bfloat16),
                pltpu.VMEM((STEPS + 1, rows, rows), jnp.float32),
                pltpu.VMEM((STEPS + 1, n_chan - 1, own, rows), jnp.float32),
                pltpu.VMEM((n_chan, 8, 128), jnp.float32),
                pltpu.SemaphoreType.DMA((STEPS + 1,)),
                pltpu.SemaphoreType.DMA((STEPS + 1,)),
                pltpu.SemaphoreType.DMA((STEPS + 1, n_chan - 1)),
                pltpu.SemaphoreType.DMA((STEPS + 1, n_chan - 1)),
                pltpu.SemaphoreType.DMA((n_chan - 1,)),
                pltpu.SemaphoreType.DMA((n_chan - 1,)),
            ],
            compiler_params=pltpu.CompilerParams(collective_id=0, has_side_effects=True),
        )(lengths, series)
        return peak.reshape(rows)

    return jax.shard_map(
        body, mesh=mesh, in_specs=(P("chan", "tm"), P()), out_specs=P("tm"), check_vma=False)
```

```python
import functools

import jax
import jax.numpy as jnp
from jax import lax
from jax.experimental import pallas as pl
from jax.experimental.pallas import tpu as pltpu
from jax.sharding import PartitionSpec as P

WIN = 256
STEPS = 2
GROUP = 16
EPS = 1e-05
MASKED = -1000000000.0
MESH = pl.DeviceIdType.MESH


def kernel(n_tm, n_chan, lengths, series, out, halo, xt, moments, mu, sc, z0, z1, z2, acc, recvbuf, peaks,
           halo_send, halo_recv, part_send, part_recv, peak_send, peak_recv):
    depth, rows = series.shape
    own = rows // n_chan
    total = rows * n_tm
    excl = WIN // 4
    block = lax.axis_index("tm")
    part = lax.axis_index("chan")

    def at(distance):
        return lax.rem(block + distance + n_tm, n_tm)

    def peer(d):
        return lax.rem(part + d, n_chan)

    barrier = pltpu.get_barrier_semaphore()
    greet = [(at(d), part) for d in (1, -1, -2)] + [(block, peer(d)) for d in range(1, n_chan)]
    for target in greet:
        pl.semaphore_signal(barrier, inc=1, device_id=target, device_id_type=MESH)
    pl.semaphore_wait(barrier, len(greet))

    halo_copies = []
    for slot, distance in enumerate((-1, 1, 2)):
        copy = pltpu.make_async_remote_copy(
            src_ref=series, dst_ref=halo.at[slot], send_sem=halo_send.at[slot], recv_sem=halo_recv.at[slot],
            device_id=(at(distance), part), device_id_type=MESH)
        copy.start()
        halo_copies.append(copy)

    half = WIN // 2
    reach = rows + half
    chunks = half // GROUP
    windows = (z0, z1, z2)

    def prepare(step):
        halo_copies[step].wait_recv()
        if step == 0:
            here, after = series[...], jnp.where(block == n_tm - 1, 0.0, halo[0])
        else:
            here, after = halo[step], series[...] if step == 1 else halo[1]
        x = jnp.concatenate([here, after], axis=1)
        xt[0:reach, :] = jnp.concatenate([x[:, :reach], x[:, half:half + reach]], axis=0).T
        span, source = 1, None
        while span < half:
            count = min(reach, -(-(reach - 2 * span) // 8) * 8)
            target = 0 if source is None else 1 - source
            mean_ref = xt if source is None else moments.at[source, 0]
            mean, later = mean_ref[0:count, :], mean_ref[span:span + count, :]
            gap = later - mean
            second = gap * gap * (span * 0.5)
            if source is not None:
                second = second + (moments[source, 1, 0:count, :] + moments[source, 1, span:span + count, :])
            moments[target, 0, 0:count, :] = (mean + later) * 0.5
            moments[target, 1, 0:count, :] = second
            span, source = 2 * span, target
        mean, second = moments[source, 0, 0:rows, :], moments[source, 1, 0:rows, :]
        later = pltpu.roll(mean, depth, 1)
        gap = later - mean
        second = second + pltpu.roll(second, depth, 1) + gap * gap * (half * 0.5)
        mu[...] = (mean + later) * 0.5
        sc[...] = lax.rsqrt(second * (1.0 / WIN) + EPS)

    def build(step, g):
        for tile in range(0, rows, 16):
            m, s = mu[tile:tile + 16, :], sc[tile:tile + 16, :]
            for k in range(GROUP):
                z = (xt[pl.ds(g * GROUP + (tile + k), 16), :] - m) * s
                windows[step][g, tile:tile + 16, 2 * depth * k:2 * depth * (k + 1)] = z.astype(jnp.bfloat16)

    def multiply(step, g):
        acc[step] += lax.dot_general(z0[g], windows[step][g], (((1,), (1,)), ((), ())),
                                     preferred_element_type=jnp.float32)

    def send(step):
        copies = []
        for d in range(1, n_chan):
            copy = pltpu.make_async_remote_copy(
                src_ref=acc.at[step, pl.ds(pl.multiple_of(peer(d) * own, own), own), :],
                dst_ref=recvbuf.at[step, d - 1],
                send_sem=part_send.at[step, d - 1], recv_sem=part_recv.at[step, d - 1],
                device_id=(block, peer(d)), device_id_type=MESH)
            copy.start()
            copies.append(copy)
        return copies

    acc[...] = jnp.zeros_like(acc)
    xt[reach:, :] = jnp.zeros((xt.shape[0] - reach, xt.shape[1]), jnp.float32)
    moments[:, :, reach:, :] = jnp.zeros((2, 2, xt.shape[0] - reach, xt.shape[1]), jnp.float32)
    sent = []
    for step in range(STEPS + 2):
        if step <= STEPS:
            prepare(step)

        def chunk(g, carry, step=step):
            if step > 0:
                multiply(step - 1, g)
            if step <= STEPS:
                build(step, g)
            return carry

        lax.fori_loop(0, chunks, chunk, 0)
        if step > 0:
            sent.append(send(step - 1))

    seg_len = rows // 2
    row_at = part * own + lax.broadcasted_iota(jnp.int32, (own, rows), 0)
    col_at = lax.broadcasted_iota(jnp.int32, (own, rows), 1)

    def valid(which, local):
        limit = jnp.where(local < seg_len, lengths[which * 2], lengths[which * 2 + 1])
        offset = jnp.where(local < seg_len, local, local - seg_len)
        return (offset < limit) & (which * rows + local <= total - WIN)

    rows_ok = valid(block, row_at)
    best = jnp.full((own, rows), MASKED, jnp.float32)
    for step in range(STEPS + 1):
        other = block - step
        safe = jnp.maximum(other, 0)
        keep = rows_ok & valid(safe, col_at) & (other >= 0) & (step * rows + row_at - col_at >= excl)
        summed = acc[step, pl.ds(pl.multiple_of(part * own, own), own), :]
        for d in range(1, n_chan):
            sent[step][d - 1].wait_recv()
            summed = summed + recvbuf[step, d - 1]
        best = jnp.maximum(best, jnp.where(keep, summed * (1.0 / WIN), MASKED))
    folded = best[:, :128]
    for at_lane in range(128, rows, 128):
        folded = jnp.maximum(folded, best[:, at_lane:at_lane + 128])
    top = jnp.max(folded.T, axis=0, keepdims=True)
    top = jnp.where(top > 0.5 * MASKED, top, 0.0)
    padded = jnp.concatenate([top, jnp.zeros((1, 128 - own), jnp.float32)], axis=1)
    peaks[0] = jnp.broadcast_to(padded, (8, 128))
    copies = []
    for d in range(1, n_chan):
        copy = pltpu.make_async_remote_copy(
            src_ref=peaks.at[0], dst_ref=peaks.at[d],
            send_sem=peak_send.at[d - 1], recv_sem=peak_recv.at[d - 1],
            device_id=(block, peer(d)), device_id_type=MESH)
        copy.start()
        copies.append(copy)
    for copy in copies:
        copy.wait_recv()
    slots = [peaks[d, 0:1, :own] for d in range(n_chan)]
    pieces = []
    for q in range(n_chan):
        piece = slots[0]
        for d in range(1, n_chan):
            piece = jnp.where(lax.rem(part + n_chan - d, n_chan) == q, slots[d], piece)
        pieces.append(piece)
    out[...] = jnp.concatenate(pieces, axis=1)

    for copy in halo_copies + [c for step in sent for c in step] + copies:
        copy.wait_send()


def solution(mesh):
    n_tm, n_chan = mesh.shape["tm"], mesh.shape["chan"]

    def body(series, lengths):
        depth, rows = series.shape
        own = rows // n_chan
        vmem = pl.BlockSpec(memory_space=pltpu.VMEM)
        peak = pl.pallas_call(
            functools.partial(kernel, n_tm, n_chan),
            out_shape=jax.ShapeDtypeStruct((1, rows), jnp.float32),
            in_specs=[pl.BlockSpec(memory_space=pltpu.SMEM), vmem],
            out_specs=vmem,
            scratch_shapes=[
                pltpu.VMEM((STEPS + 1, depth, rows), jnp.float32),
                pltpu.VMEM((rows + WIN // 2 + 16, 2 * depth), jnp.float32),
                pltpu.VMEM((2, 2, rows + WIN // 2 + 16, 2 * depth), jnp.float32),
                pltpu.VMEM((rows, 2 * depth), jnp.float32),
                pltpu.VMEM((rows, 2 * depth), jnp.float32),
                pltpu.VMEM((WIN // 2 // GROUP, rows, GROUP * 2 * depth), jnp.bfloat16),
                pltpu.VMEM((WIN // 2 // GROUP, rows, GROUP * 2 * depth), jnp.bfloat16),
                pltpu.VMEM((WIN // 2 // GROUP, rows, GROUP * 2 * depth), jnp.bfloat16),
                pltpu.VMEM((STEPS + 1, rows, rows), jnp.float32),
                pltpu.VMEM((STEPS + 1, n_chan - 1, own, rows), jnp.float32),
                pltpu.VMEM((n_chan, 8, 128), jnp.float32),
                pltpu.SemaphoreType.DMA((STEPS + 1,)),
                pltpu.SemaphoreType.DMA((STEPS + 1,)),
                pltpu.SemaphoreType.DMA((STEPS + 1, n_chan - 1)),
                pltpu.SemaphoreType.DMA((STEPS + 1, n_chan - 1)),
                pltpu.SemaphoreType.DMA((n_chan - 1,)),
                pltpu.SemaphoreType.DMA((n_chan - 1,)),
            ],
            compiler_params=pltpu.CompilerParams(collective_id=0, has_side_effects=True),
        )(lengths, series)
        return peak.reshape(rows)

    return jax.shard_map(
        body, mesh=mesh, in_specs=(P("chan", "tm"), P()), out_specs=P("tm"), check_vma=False)
```
